128 devices in a mesh: grp: 8 (over x, core), row: 16 (over z, y).
Axes of the slice: x: 4, y: 4, z: 4, core: 2. Of those that a mesh axis runs over, the one named last changes fastest.
Arguments:
- iterate: bfloat16 [64, 1048576], P(None, ('grp', 'row')), may hold values from -6 to 6
- near_tiles: bfloat16 [8192, 128, 128], P(('grp', 'row')), may hold values from -0.125 to 0.125
- near_rows: int32 [8192], P(('grp', 'row')), may hold values from 0 to 63
- near_cols: int32 [8192], P(('grp', 'row')), may hold values from 0 to 63
- near_count: int32 [128], P(('grp', 'row')), may hold values from 32 to 64, as said below
- cross_tiles: bfloat16 [8192, 128, 128], P(('grp', 'row')), may hold values from -0.125 to 0.125
- cross_rows: int32 [8192], P(('grp', 'row')), may hold values from 0 to 63
- cross_cols: int32 [8192], P(('grp', 'row')), may hold values from 0 to 63
- cross_count: int32 [128], P(('grp', 'row')), may hold values from 0 to 64, as said below
Outputs:
- basis: float32 [64, 1048576], P(None, ('grp', 'row'))
- rayleigh: float32 [64, 64], replicated
The draws below stay inside these ranges and needn't reach their ends.
Inputs may be any that keep to these rules, and one draw needn't show every extreme that they name: `near_count`: slots at or past a device's count hold no part of the matrix. Some device uses all 64 near slots. `cross_count`: the last device's count is 0; some other device uses all 64 cross slots. `near_rows`: positions may repeat; repeated tiles add.
All inputs are finite; a program needn't handle non-finite values.
Results may differ from the reference program's by a relative error of at most 0.003.
Values may be sent and summed in bfloat16 or wider, within the bound.
No kernel may reach another device: no remote copies, remote signals or barrier semaphores. Data moves between devices by JAX's collectives and lax.ppermute only.
A program may use at most 128 MiB of HBM per device.

```python
import jax
import jax.numpy as jnp
from jax import lax

EIGS = 64
TILE = 128
BR_DEV = 64
NEAR_DEV = 64
CROSS_DEV = 64
NROWS = 1048576
DEVICES = 128


def draw_near_count(key, part):
    counts = jax.random.randint(key, (DEVICES,), NEAR_DEV // 2, NEAR_DEV + 1)
    fullest = jax.random.randint(jax.random.fold_in(key, 7), (), 0, DEVICES)
    counts = jnp.where(jnp.arange(DEVICES) == fullest, NEAR_DEV, counts)
    return counts.astype(jnp.int32)


def draw_cross_count(key, part):
    counts = jax.random.randint(jax.random.fold_in(key, 11), (DEVICES,), CROSS_DEV // 2, CROSS_DEV + 1)
    fullest = jax.random.randint(jax.random.fold_in(key, 13), (), 0, DEVICES - 1)
    places = jnp.arange(DEVICES)
    counts = jnp.where(places == fullest, CROSS_DEV, counts)
    counts = jnp.where(places == DEVICES - 1, 0, counts)
    return counts.astype(jnp.int32)


def plant(array, key, least, top_value):
    index_at = [jax.random.randint(jax.random.fold_in(key, axis), (), 0, length) for axis, length in enumerate(array.shape)]
    main_axis = array.shape.index(max(array.shape))
    neighbour = index_at[:main_axis] + [(index_at[main_axis] + 1) % array.shape[main_axis]] + index_at[main_axis + 1:]
    return array.at[tuple(index_at)].set(least).at[tuple(neighbour)].set(top_value)


def levels(key, dims, pieces, least, high):
    level = 1.0
    for axis_at, parts in pieces:
        steps = jax.random.uniform(jax.random.fold_in(jax.random.fold_in(key, 6), axis_at), (parts,), jnp.float32, least / len(pieces), high / len(pieces))
        level = level * jnp.repeat(jnp.exp(steps), dims[axis_at] // parts).reshape((-1,) + (1,) * (len(dims) - 1 - axis_at))
    return level


def noise(rng, extent, scale, bound, pieces=(), held_as=jnp.bfloat16):
    array = jax.random.normal(rng, extent, jnp.float32) * scale
    if len(pieces) > 0:
        array = levels(rng, extent, pieces, -0.22, 0.18) * array
    return jnp.clip(array, min=-bound, max=bound).astype(held_as)


def setup_inputs(seed: int = 0) -> dict:
    splits = jax.random.split(jax.random.key(seed), 10)
    return {
        "iterate": noise(splits[0], (EIGS, NROWS), 1.0, 6.0, ((1, 128),)),
        "near_tiles": noise(splits[1], (DEVICES * NEAR_DEV, TILE, TILE), (32 * NEAR_DEV) ** -0.5, 0.125, ((0, 128),)),
        "near_rows": plant(jax.random.randint(splits[2], (DEVICES * NEAR_DEV,), 0, BR_DEV), jax.random.fold_in(splits[2], 1), 0, BR_DEV - 1).astype(jnp.int32),
        "near_cols": plant(jax.random.randint(splits[3], (DEVICES * NEAR_DEV,), 0, BR_DEV), jax.random.fold_in(splits[3], 1), 0, BR_DEV - 1).astype(jnp.int32),
        "near_count": draw_near_count(jax.random.fold_in(splits[9], 71), 0),
        "cross_tiles": noise(splits[5], (DEVICES * CROSS_DEV, TILE, TILE), (32 * NEAR_DEV) ** -0.5, 0.125, ((0, 128),)),
        "cross_rows": plant(jax.random.randint(splits[6], (DEVICES * CROSS_DEV,), 0, BR_DEV), jax.random.fold_in(splits[6], 1), 0, BR_DEV - 1).astype(jnp.int32),
        "cross_cols": plant(jax.random.randint(splits[7], (DEVICES * CROSS_DEV,), 0, BR_DEV), jax.random.fold_in(splits[7], 1), 0, BR_DEV - 1).astype(jnp.int32),
        "cross_count": draw_cross_count(jax.random.fold_in(splits[9], 71), 0),
    }


def tile_terms(blocks, index, tiles, flipped):
    picked = jnp.take(blocks, index, axis=1)
    if flipped:
        return jnp.einsum('ktr,trc->tkc', picked, tiles, precision=lax.Precision.HIGHEST)
    return jnp.einsum('ktc,trc->tkr', picked, tiles, precision=lax.Precision.HIGHEST)

def place(terms, index, weight):
    placed = jax.ops.segment_sum(terms * weight[:, None, None], index, num_segments=BR_DEV)
    return jnp.transpose(placed, (1, 0, 2)).reshape(EIGS, BR_DEV * TILE)

def reference(iterate, near_tiles, near_rows, near_cols, near_count, cross_tiles, cross_rows, cross_cols, cross_count):
    width = BR_DEV * TILE

    def apply_s(vector_b):
        blocks = vector_b.astype(jnp.float32).reshape(EIGS, DEVICES, BR_DEV, TILE)

        def per_device(dev):
            own = lax.dynamic_index_in_dim(blocks, dev, 1, keepdims=False)
            after = jnp.minimum(dev + 1, DEVICES - 1).astype(jnp.int32)
            ahead = lax.dynamic_index_in_dim(blocks, after, 1, keepdims=False)
            ntiles = lax.dynamic_slice_in_dim(near_tiles, dev * NEAR_DEV, NEAR_DEV, 0).astype(jnp.float32)
            nrows = lax.dynamic_slice_in_dim(near_rows, dev * NEAR_DEV, NEAR_DEV, 0)
            ncols = lax.dynamic_slice_in_dim(near_cols, dev * NEAR_DEV, NEAR_DEV, 0)
            ncount = lax.dynamic_index_in_dim(near_count, dev, 0, keepdims=False)
            nmask = (jnp.arange(NEAR_DEV, dtype=jnp.int32) < ncount).astype(jnp.float32)
            ctiles = lax.dynamic_slice_in_dim(cross_tiles, dev * CROSS_DEV, CROSS_DEV, 0).astype(jnp.float32)
            crows = lax.dynamic_slice_in_dim(cross_rows, dev * CROSS_DEV, CROSS_DEV, 0)
            ccols = lax.dynamic_slice_in_dim(cross_cols, dev * CROSS_DEV, CROSS_DEV, 0)
            ccount = lax.dynamic_index_in_dim(cross_count, dev, 0, keepdims=False)
            cmask = (jnp.arange(CROSS_DEV, dtype=jnp.int32) < ccount).astype(jnp.float32)
            total = place(tile_terms(own, ncols, ntiles, False), nrows, nmask)
            total = total + place(tile_terms(own, nrows, ntiles, True), ncols, nmask)
            total = total + place(tile_terms(ahead, ccols, ctiles, False), crows, cmask)
            later = place(tile_terms(own, crows, ctiles, True), ccols, cmask)
            return (total, later)
        own_all, later_all = lax.map(per_device, jnp.arange(DEVICES, dtype=jnp.int32))
        moved = jnp.concatenate([jnp.zeros_like(later_all[:1]), later_all[:-1]], 0)
        summed = own_all + moved
        return jnp.transpose(summed, (1, 0, 2)).reshape(EIGS, DEVICES * width)

    def mapped(current):
        return (-0.25 * current - apply_s(current.astype(jnp.bfloat16))) / 0.75
    before = iterate.astype(jnp.float32)
    current = mapped(before)
    for step in range(3):
        following = 2.0 * mapped(current) - before
        before, current = (current, following)
    rounded = current.astype(jnp.bfloat16)
    rounded_f = rounded.astype(jnp.float32)
    image = rounded_f - apply_s(rounded)
    count_rows = float(DEVICES * width)
    gram = jnp.dot(current.astype(jnp.float32), current.T.astype(jnp.float32), precision=lax.Precision.HIGHEST, preferred_element_type=jnp.float32) / count_rows
    projected = jnp.dot(rounded_f.astype(jnp.float32), image.T.astype(jnp.float32), precision=lax.Precision.HIGHEST, preferred_element_type=jnp.float32) / count_rows
    lower = jnp.linalg.cholesky(gram)
    basis = jax.scipy.linalg.solve_triangular(lower, current, lower=True)
    halfway = jax.scipy.linalg.solve_triangular(lower, projected, lower=True)
    rayleigh = jax.scipy.linalg.solve_triangular(lower, halfway.T, lower=True)
    return (basis, rayleigh)
```

```python
import jax
import jax.numpy as jnp
from jax import lax
from jax.experimental import pallas as pl
from jax.experimental.pallas import tpu as pltpu
from jax.sharding import Mesh
from jax.sharding import PartitionSpec as P

EIGS = 64
TILE = 128
BR_DEV = 64
SLOTS = 64
HALF = 32
CHUNK = 16
PANEL = 1024
AXES = ("grp_0", "grp_1", "row_0", "row_1")
F32 = jnp.float32
BF16 = jnp.bfloat16
VM = pl.BlockSpec(memory_space=pltpu.VMEM)
SM = pl.BlockSpec(memory_space=pltpu.SMEM)
PARAMS = pltpu.CompilerParams(vmem_limit_bytes=16 * 1024 * 1024)
NEAR_ROW, NEAR_COL, CROSS_ROW, CROSS_COL, COUNTS = 0, 1, 2, 3, 4


def call(body, shapes, inputs, scratch=()):
    specs = [SM] + [VM] * (len(inputs) - 1)
    return pl.pallas_call(
        body,
        out_shape=[jax.ShapeDtypeStruct(s, d) for s, d in shapes],
        in_specs=specs,
        out_specs=[VM] * len(shapes),
        scratch_shapes=[pltpu.VMEM(s, d) for s, d in scratch],
        compiler_params=PARAMS,
        name=body.__name__,
    )(*inputs)


def block(i):
    return pl.ds(pl.multiple_of(i * TILE, TILE), TILE)


def dot(a, b):
    return jnp.dot(a, b, preferred_element_type=F32)


def dot_t(a, b):
    return lax.dot_general(a, b, (((1,), (1,)), ((), ())), preferred_element_type=F32)


def over_slots(count, body):
    def chunk(i, carry):
        for u in range(CHUNK):
            body(i * CHUNK + u)
        return carry

    lax.fori_loop(0, (count + CHUNK - 1) // CHUNK, chunk, 0)


def over_panels(body):
    def panel(i, carry):
        body(pl.ds(pl.multiple_of(i * PANEL, PANEL), PANEL))
        return carry

    lax.fori_loop(0, BR_DEV * TILE // PANEL, panel, 0)


def lent(idx, tiles, source, acc, out):
    count = idx[COUNTS, 1]
    acc[...] = jnp.zeros_like(acc)

    def slot(t):
        left = source[:, block(idx[CROSS_ROW, t])]
        acc[:, block(idx[CROSS_COL, t])] += dot(left, tiles[t])

    over_slots(count, slot)

    def close(s):
        out[:, s] = acc[:, s].astype(BF16)

    over_panels(close)


def first_lent(idx, cross, source, out_a, out_b, acc):
    count = idx[COUNTS, 1]
    acc[...] = jnp.zeros_like(acc)

    def slot(t):
        left = source[:, block(idx[CROSS_ROW, t])]
        left = jnp.where(t < count, left, jnp.zeros_like(left))
        acc[:, block(idx[CROSS_COL, t])] += dot(left, cross[t])

    over_slots(count, slot)

    def close(s):
        out_a[:, s] = acc[:HALF, s].astype(BF16)
        out_b[:, s] = acc[HALF:, s].astype(BF16)

    over_panels(close)


def prepare(idx, near, cross, near_m, near_t, cross_m, cross_t):
    def one(t, carry):
        for which, src, plain, flipped in ((0, near, near_m, near_t), (1, cross, cross_m, cross_t)):
            tile = src[t]
            tile = jnp.where(t < idx[COUNTS, which], tile, jnp.zeros_like(tile))
            plain[t] = tile
            flipped[t] = tile.T
        return carry

    lax.fori_loop(0, SLOTS, one, 0)


def products(idx, near_m, near_t, cross_t, own, ahead, to_row, to_col, from_ahead):
    to_row[...] = jnp.zeros_like(to_row)
    to_col[...] = jnp.zeros_like(to_col)
    from_ahead[...] = jnp.zeros_like(from_ahead)
    most = jnp.maximum(idx[COUNTS, 0], idx[COUNTS, 1])

    def slot(t):
        row, col = idx[NEAR_ROW, t], idx[NEAR_COL, t]
        to_row[:, block(row)] += dot(own[:, block(col)], near_t[t])
        to_col[:, block(col)] += dot(own[:, block(row)], near_m[t])
        from_ahead[:, block(idx[CROSS_ROW, t])] += dot(
            ahead[:, block(idx[CROSS_COL, t])], cross_t[t]
        )

    over_slots(most, slot)


def first_step(
    idx, near_m, near_t, cross_m, cross_t, own, ahead, behind, new, new_b, new_w, s0, s1, s2
):
    products(idx, near_m, near_t, cross_t, own, ahead, s0, s1, s2)

    def update(s):
        image = s0[:, s] + s1[:, s] + s2[:, s] + behind[:, s].astype(F32)
        following = (-0.25 * own[:, s].astype(F32) - image) * (1.0 / 0.75)
        new[:, s] = following
        new_b[:, s] = following.astype(BF16)

    over_panels(update)
    lent(idx, cross_m, new_b, s0, new_w)


def middle_step(
    idx, near_m, near_t, cross_m, cross_t, own, ahead, behind, current, before,
    new, new_b, new_w, s0, s1, s2,
):
    products(idx, near_m, near_t, cross_t, own, ahead, s0, s1, s2)

    def update(s):
        image = s0[:, s] + s1[:, s] + s2[:, s] + behind[:, s].astype(F32)
        following = (-0.25 * current[:, s] - image) * (2.0 / 0.75) - before[:, s].astype(F32)
        new[:, s] = following
        new_b[:, s] = following.astype(BF16)

    over_panels(update)
    lent(idx, cross_m, new_b, s0, new_w)


def last_step(
    idx, near_m, near_t, cross_m, cross_t, own, ahead, behind, current, before,
    rest, new_b, new_w, s0, s1, s2,
):
    products(idx, near_m, near_t, cross_t, own, ahead, s0, s1, s2)

    def update(s):
        image = s0[:, s] + s1[:, s] + s2[:, s] + behind[:, s].astype(F32)
        following = (-0.25 * current[:, s] - image) * (2.0 / 0.75) - before[:, s].astype(F32)
        rounded = following.astype(BF16)
        new_b[:, s] = rounded
        rest[:, s] = (following - rounded.astype(F32)).astype(BF16)

    over_panels(update)
    lent(idx, cross_m, new_b, s0, new_w)


def local_sums(idx, near_m, own_a, own_b, rest_a, rest_b, out, acc):
    acc[...] = jnp.zeros_like(acc)

    def slot(t):
        row, col = idx[NEAR_ROW, t], idx[NEAR_COL, t]
        left = jnp.concatenate([own_a[:, block(row)], own_b[:, block(row)]], axis=0)
        acc[:, block(col)] += dot(left, near_m[t])

    over_slots(idx[COUNTS, 0], slot)
    total = jnp.zeros((3 * EIGS, EIGS), F32)
    for k in range(0, BR_DEV * TILE, PANEL):
        s = slice(k, k + PANEL)
        own = jnp.concatenate([own_a[:, s], own_b[:, s]], axis=0)
        left = jnp.concatenate(
            [own, rest_a[:, s], rest_b[:, s], acc[:, s].astype(BF16)], axis=0
        )
        total = total + dot_t(left, own)
    half = 0.5 * total[:EIGS]
    out[:, :EIGS] = half + total[EIGS : 2 * EIGS]
    out[:, EIGS:] = half - total[2 * EIGS :]


def crossing_sums(
    idx, sums, own_a, own_b, lent_a, lent_b, ahead_a, ahead_b, behind_a, behind_b, out
):
    middle = BR_DEV * TILE // 2
    total = jnp.zeros((EIGS, EIGS), F32)
    for k in range(0, middle, PANEL):
        s = slice(k, k + PANEL)
        left = jnp.concatenate([behind_a[:, s], behind_b[:, s]], axis=0)
        total = total + dot_t(left, jnp.concatenate([own_a[:, s], own_b[:, s]], axis=0))
        u = slice(middle + k, middle + k + PANEL)
        left = jnp.concatenate([lent_a[:, u], lent_b[:, u]], axis=0)
        total = total + dot_t(left, jnp.concatenate([ahead_a[:, s], ahead_b[:, s]], axis=0))
    gram = sums[:, :EIGS]
    inner = sums[:, EIGS:] - total
    out[:, :EIGS] = gram + gram.T
    out[:, EIGS:] = inner + inner.T


def split(x):
    high = x.astype(BF16)
    return high, (x - high.astype(F32)).astype(BF16)


def finish(idx, sums, own_a, own_b, rest_a, rest_b, basis, rayleigh):
    count = 1.0 / float(128 * BR_DEV * TILE)
    rows = lax.broadcasted_iota(jnp.int32, (EIGS, 2 * EIGS), 0)
    lanes = lax.broadcasted_iota(jnp.int32, (EIGS, 2 * EIGS), 1)
    work = jnp.where(lanes < EIGS, sums[...] * count, (lanes - EIGS == rows).astype(F32))
    for j in range(EIGS - 1):
        pivot_row = work[j : j + 1, :] / work[j : j + 1, j : j + 1]
        column = jnp.where(rows[:, :1] > j, work[:, j : j + 1], 0.0)
        work = work - column * pivot_row
    pivots = jnp.sum(jnp.where(lanes == rows, work, 0.0), axis=1, keepdims=True)
    inverse = (work / jnp.sqrt(pivots))[:, EIGS:]
    high, low = split(inverse)
    left = jnp.concatenate([high, high, low], axis=1)
    for k in range(0, BR_DEV * TILE, PANEL):
        s = slice(k, k + PANEL)
        own = [own_a[:, s], own_b[:, s]]
        right = jnp.concatenate(own + [rest_a[:, s], rest_b[:, s]] + own, axis=0)
        basis[:, s] = dot(left, right)
    inner = sums[:, EIGS:] * count
    halfway = jnp.dot(
        inverse, inner, precision=lax.Precision.HIGHEST, preferred_element_type=F32
    )
    rayleigh[...] = lax.dot_general(
        inverse,
        halfway,
        (((1,), (1,)), ((), ())),
        precision=lax.Precision.HIGHEST,
        preferred_element_type=F32,
    )


def shards(
    iterate, near, near_rows, near_cols, near_count, cross, cross_rows, cross_cols, cross_count
):
    devices = lax.axis_size(AXES)
    width = BR_DEV * TILE
    onward = [(i, i + 1) for i in range(devices - 1)]
    back = [(b, a) for a, b in onward]

    def to_next(x):
        return lax.ppermute(x, AXES, onward)

    def to_last(x):
        return lax.ppermute(x, AXES, back)

    counts = jnp.concatenate([near_count, cross_count, jnp.zeros((SLOTS - 2,), jnp.int32)])
    idx = jnp.stack([near_rows, near_cols, cross_rows, cross_cols, counts])

    half = ((HALF, width), BF16)
    full = ((HALF, width), F32)
    tiles = ((SLOTS, TILE, TILE), BF16)

    own = [iterate[:HALF], iterate[HALF:]]
    ahead = [to_last(x) for x in own]
    give = call(first_lent, [half, half], (idx, cross, iterate), [((EIGS, width), F32)])
    behind = [to_next(x) for x in give]
    near_m, near_t, cross_m, cross_t = call(prepare, [tiles] * 4, (idx, near, cross))
    operands = (idx, near_m, near_t, cross_m, cross_t)

    before, current = [None, None], [x for x in own]
    lend = [None, None]
    rest = [None, None]
    for step in range(4):
        for h in range(2):
            args = operands + (own[h], ahead[h], behind[h])
            if step == 0:
                new, new_b, new_w = call(first_step, [full, half, half], args, [full] * 3)
                before[h], current[h] = own[h], new
            elif step < 3:
                args = args + (current[h], before[h])
                new, new_b, new_w = call(middle_step, [full, half, half], args, [full] * 3)
                before[h], current[h] = current[h], new
            else:
                args = args + (current[h], before[h])
                rest[h], new_b, new_w = call(last_step, [half, half, half], args, [full] * 3)
            own[h], lend[h] = new_b, new_w
            if step < 3:
                ahead[h], behind[h] = to_last(new_b), to_next(new_w)
            else:
                ahead[h] = to_last(new_b[:, width // 2 :])
                behind[h] = to_next(new_w[:, : width // 2])

    sums = call(
        local_sums,
        [((EIGS, 2 * EIGS), F32)],
        (idx, near_m, *own, *rest),
        [((EIGS, width), F32)],
    )[0]
    sums = call(
        crossing_sums,
        [((EIGS, 2 * EIGS), F32)],
        (idx, sums, *own, *lend, *ahead, *behind),
    )[0]
    reach = 1
    while reach < devices:
        sums = sums + lax.ppermute(sums, AXES, [(i, i ^ reach) for i in range(devices)])
        reach *= 2
    basis, rayleigh = call(
        finish,
        [((EIGS, width), F32), ((EIGS, EIGS), F32)],
        (idx, sums, *own, *rest),
    )
    return basis, rayleigh


def solution(mesh):
    finer = Mesh(mesh.devices.reshape(4, 2, 4, 4), AXES)
    in_specs = (
        P(None, AXES),
        P(AXES, None, None),
        P(AXES),
        P(AXES),
        P(AXES),
        P(AXES, None, None),
        P(AXES),
        P(AXES),
        P(AXES),
    )
    return jax.shard_map(
        shards, mesh=finer, in_specs=in_specs, out_specs=(P(None, AXES), P()), check_vma=False
    )
```

```python
import jax
import jax.numpy as jnp
from jax import lax
from jax.experimental import pallas as pl
from jax.experimental.pallas import tpu as pltpu
from jax.sharding import Mesh
from jax.sharding import PartitionSpec as P

EIGS = 64
TILE = 128
BR_DEV = 64
SLOTS = 64
HALF = 32
CHUNK = 32
PANEL = 1024
AXES = ("grp_0", "grp_1", "row_0", "row_1")
F32 = jnp.float32
BF16 = jnp.bfloat16
VM = pl.BlockSpec(memory_space=pltpu.VMEM)
SM = pl.BlockSpec(memory_space=pltpu.SMEM)
PARAMS = pltpu.CompilerParams(vmem_limit_bytes=16 * 1024 * 1024)
NEAR_ROW, NEAR_COL, CROSS_ROW, CROSS_COL, COUNTS = 0, 1, 2, 3, 4


def call(body, shapes, inputs, scratch=(), aliases=None, scalars=True):
    specs = [SM if scalars else VM] + [VM] * (len(inputs) - 1)
    return pl.pallas_call(
        body,
        out_shape=[jax.ShapeDtypeStruct(s, d) for s, d in shapes],
        in_specs=specs,
        out_specs=[VM] * len(shapes),
        scratch_shapes=[pltpu.VMEM(s, d) for s, d in scratch],
        input_output_aliases=aliases or {},
        compiler_params=PARAMS,
    )(*inputs)


def block(i):
    return pl.ds(pl.multiple_of(i * TILE, TILE), TILE)


def dot(a, b):
    return jnp.dot(a, b, preferred_element_type=F32)


def dot_t(a, b):
    return lax.dot_general(a, b, (((1,), (1,)), ((), ())), preferred_element_type=F32)


def over_slots(count, body):
    def chunk(i, carry):
        for u in range(0, CHUNK, 2):
            body(i * CHUNK + u, i * CHUNK + u + 1)
        return carry

    lax.fori_loop(0, (count + CHUNK - 1) // CHUNK, chunk, 0)


def over_panels(body):
    def panel(i, carry):
        body(pl.ds(pl.multiple_of(i * PANEL, PANEL), PANEL))
        return carry

    lax.fori_loop(0, BR_DEV * TILE // PANEL, panel, 0)


def add_pair(acc, to_1, to_2, left_1, left_2, tile_1, tile_2):
    rows = left_1.shape[0]
    both = dot(
        jnp.concatenate([left_1, left_2], axis=0), jnp.concatenate([tile_1, tile_2], axis=1)
    )
    acc[:, block(to_1)] += both[:rows, :TILE]
    acc[:, block(to_2)] += both[rows:, TILE:]


def add_products(idx, count, source, source_at, target, target_at, tiles):
    def pair(t, u):
        add_pair(
            target,
            idx[target_at, t],
            idx[target_at, u],
            source[:, block(idx[source_at, t])],
            source[:, block(idx[source_at, u])],
            tiles[t],
            tiles[u],
        )

    over_slots(count, pair)


def first_lent(idx, cross, source, out_a, out_b, acc):
    count = idx[COUNTS, 1]
    acc[...] = jnp.zeros_like(acc)

    def left(t):
        rows = source[:, block(idx[CROSS_ROW, t])]
        return jnp.where(t < count, rows, jnp.zeros_like(rows))

    def pair(t, u):
        add_pair(
            acc, idx[CROSS_COL, t], idx[CROSS_COL, u], left(t), left(u), cross[t], cross[u]
        )

    over_slots(count, pair)

    def close(s):
        out_a[:, s] = acc[:HALF, s].astype(BF16)
        out_b[:, s] = acc[HALF:, s].astype(BF16)

    over_panels(close)


def prepare(idx, near, cross, near_m, near_t, cross_m, cross_t):
    def one(t, carry):
        for which, src, plain, flipped in ((0, near, near_m, near_t), (1, cross, cross_m, cross_t)):
            tile = src[t]
            tile = jnp.where(t < idx[COUNTS, which], tile, jnp.zeros_like(tile))
            plain[t] = tile
            flipped[t] = tile.T
        return carry

    lax.fori_loop(0, SLOTS, one, 0)


def near_part(idx, near_m, near_t, own, to_row, to_col):
    to_row[...] = jnp.zeros_like(to_row)
    to_col[...] = jnp.zeros_like(to_col)

    def pair(t, u):
        for acc, source_at, target_at, tiles in (
            (to_row, NEAR_COL, NEAR_ROW, near_t),
            (to_col, NEAR_ROW, NEAR_COL, near_m),
        ):
            add_pair(
                acc,
                idx[target_at, t],
                idx[target_at, u],
                own[:, block(idx[source_at, t])],
                own[:, block(idx[source_at, u])],
                tiles[t],
                tiles[u],
            )

    over_slots(idx[COUNTS, 0], pair)

    def close(s):
        to_row[:, s] += to_col[:, s]

    over_panels(close)


def step_body(idx, cross_m, cross_t, ahead, behind, current, before, new, new_b, new_w, acc):
    count = idx[COUNTS, 1]
    add_products(idx, count, ahead, CROSS_COL, new, CROSS_ROW, cross_t)

    def update(s):
        image = new[:, s] + behind[:, s].astype(F32)
        following = -0.25 * current[:, s].astype(F32) - image
        if before is None:
            following = following * (1.0 / 0.75)
        else:
            following = following * (2.0 / 0.75) - before[:, s].astype(F32)
        new[:, s] = following
        new_b[:, s] = following.astype(BF16)
        acc[:, s] = jnp.zeros_like(following)

    over_panels(update)
    add_products(idx, count, new_b, CROSS_ROW, acc, CROSS_COL, cross_m)

    def close(s):
        new_w[:, s] = acc[:, s].astype(BF16)

    over_panels(close)


def first_step(idx, near_image, cross_m, cross_t, ahead, behind, current, new, new_b, new_w, acc):
    step_body(idx, cross_m, cross_t, ahead, behind, current, None, new, new_b, new_w, acc)


def next_step(
    idx, near_image, cross_m, cross_t, ahead, behind, current, before, new, new_b, new_w, acc
):
    step_body(idx, cross_m, cross_t, ahead, behind, current, before, new, new_b, new_w, acc)


def local_sums(idx, near_m, own_a, own_b, last_a, last_b, out, stack, acc):
    acc[...] = jnp.zeros_like(acc)

    def left(t):
        rows = block(idx[NEAR_ROW, t])
        return jnp.concatenate([own_a[:, rows], own_b[:, rows]], axis=0)

    def pair(t, u):
        add_pair(
            acc, idx[NEAR_COL, t], idx[NEAR_COL, u], left(t), left(u), near_m[t], near_m[u]
        )

    over_slots(idx[COUNTS, 0], pair)
    total = jnp.zeros((3 * EIGS, EIGS), F32)
    for k in range(0, BR_DEV * TILE, PANEL):
        s = slice(k, k + PANEL)
        own = jnp.concatenate([own_a[:, s], own_b[:, s]], axis=0)
        rest = jnp.concatenate([last_a[:, s], last_b[:, s]], axis=0) - own.astype(F32)
        both = jnp.concatenate([own, rest.astype(BF16)], axis=0)
        stack[:, s] = both
        total = total + dot_t(jnp.concatenate([both, acc[:, s].astype(BF16)], axis=0), own)
    half = 0.5 * total[:EIGS]
    out[:, :EIGS] = half + total[EIGS : 2 * EIGS]
    out[:, EIGS:] = half - total[2 * EIGS :]


def crossing_sums(
    sums, own_a, own_b, lent_a, lent_b, ahead_a, ahead_b, behind_a, behind_b, out
):
    middle = BR_DEV * TILE // 2
    total = jnp.zeros((EIGS, EIGS), F32)
    for k in range(0, middle, PANEL):
        s = slice(k, k + PANEL)
        left = jnp.concatenate([behind_a[:, s], behind_b[:, s]], axis=0)
        total = total + dot_t(left, jnp.concatenate([own_a[:, s], own_b[:, s]], axis=0))
        u = slice(middle + k, middle + k + PANEL)
        left = jnp.concatenate([lent_a[:, u], lent_b[:, u]], axis=0)
        total = total + dot_t(left, jnp.concatenate([ahead_a[:, s], ahead_b[:, s]], axis=0))
    gram = sums[:, :EIGS]
    inner = sums[:, EIGS:] - total
    out[:, :EIGS] = gram + gram.T
    out[:, EIGS:] = inner + inner.T


def split(x):
    high = x.astype(BF16)
    return high, (x - high.astype(F32)).astype(BF16)


def inverse_factor(gram):
    wide = 2 * EIGS
    rows = lax.broadcasted_iota(jnp.int32, (EIGS, wide), 0)
    lanes = lax.broadcasted_iota(jnp.int32, (EIGS, wide), 1)
    work = jnp.where(lanes < EIGS, gram, (lanes - EIGS == rows).astype(F32))
    work = [work[i : i + 8] for i in range(0, EIGS, 8)]
    below = lax.broadcasted_iota(jnp.int32, (8, wide), 0)
    done = []
    for p in range(EIGS // 8):
        columns = [
            [jnp.broadcast_to(w[:, 8 * p + k : 8 * p + k + 1], (8, wide)) for w in work]
            for k in range(8)
        ]
        for k in range(8):
            pivot = jnp.broadcast_to(columns[k][0][k : k + 1], (8, wide))
            row = jnp.broadcast_to(work[0][k : k + 1], (8, wide))
            scale = 1.0 / pivot
            factors = [c * scale for c in columns[k]]
            factors[0] = jnp.where(below > k, factors[0], 0.0)
            for later in range(k + 1, 8):
                top = jnp.broadcast_to(columns[later][0][k : k + 1], (8, wide))
                columns[later] = [c - f * top for c, f in zip(columns[later], factors)]
            work = [w - f * row for w, f in zip(work, factors)]
        done.append(work[0])
        work = work[1:]
    work = jnp.concatenate(done, axis=0)
    pivots = jnp.sum(jnp.where(lanes == rows, work, 0.0), axis=1, keepdims=True)
    return (work / jnp.sqrt(pivots))[:, EIGS:]


def finish(sums, stack, basis, rayleigh):
    count = 1.0 / float(128 * BR_DEV * TILE)
    inverse = inverse_factor(sums[...] * count)
    high, low = split(inverse)
    left = jnp.concatenate([high, high, low], axis=1)
    for k in range(0, BR_DEV * TILE, PANEL):
        s = slice(k, k + PANEL)
        both = stack[:, s]
        basis[:, s] = dot(left, jnp.concatenate([both, both[:EIGS]], axis=0))
    inner = sums[:, EIGS:] * count
    halfway = jnp.dot(
        inverse, inner, precision=lax.Precision.HIGHEST, preferred_element_type=F32
    )
    rayleigh[...] = lax.dot_general(
        inverse,
        halfway,
        (((1,), (1,)), ((), ())),
        precision=lax.Precision.HIGHEST,
        preferred_element_type=F32,
    )


def shards(
    iterate, near, near_rows, near_cols, near_count, cross, cross_rows, cross_cols, cross_count
):
    devices = lax.axis_size(AXES)
    width = BR_DEV * TILE
    onward = [(i, i + 1) for i in range(devices - 1)]
    back = [(b, a) for a, b in onward]

    def to_next(x):
        return lax.ppermute(x, AXES, onward)

    def to_last(x):
        return lax.ppermute(x, AXES, back)

    counts = jnp.concatenate([near_count, cross_count, jnp.zeros((SLOTS - 2,), jnp.int32)])
    idx = jnp.stack([near_rows, near_cols, cross_rows, cross_cols, counts])

    half = ((HALF, width), BF16)
    full = ((HALF, width), F32)
    tiles = ((SLOTS, TILE, TILE), BF16)
    middle = width // 2

    own = [iterate[:HALF], iterate[HALF:]]
    ahead, behind = [None, None], [None, None]
    ahead[0] = to_last(own[0])
    give = call(first_lent, [half, half], (idx, cross, iterate), [((EIGS, width), F32)])
    behind[0] = to_next(give[0])
    ahead[1] = to_last(own[1])
    behind[1] = to_next(give[1])
    near_m, near_t, cross_m, cross_t = call(prepare, [tiles] * 4, (idx, near, cross))

    def near_image(h):
        return call(near_part, [full], (idx, near_m, near_t, own[h]), [full])[0]

    images = [near_image(0), near_image(1)]
    before, current = [None, None], list(own)
    lend = [None, None]
    for step in range(4):
        for h in range(2):
            args = (idx, images[h], cross_m, cross_t, ahead[h], behind[h], current[h])
            if step == 0:
                new, new_b, new_w = call(first_step, [full, half, half], args, [full], {1: 0})
            else:
                new, new_b, new_w = call(
                    next_step, [full, half, half], args + (before[h],), [full], {1: 0}
                )
            before[h], current[h] = current[h], new
            own[h], lend[h] = new_b, new_w
            last = step == 3
            ahead[h] = to_last(new_b[:, middle:] if last else new_b)
            behind[h] = to_next(new_w[:, :middle] if last else new_w)
            if not last:
                images[h] = near_image(h)

    sums, stack = call(
        local_sums,
        [((EIGS, 2 * EIGS), F32), ((2 * EIGS, width), BF16)],
        (idx, near_m, *own, *current),
        [((EIGS, width), F32)],
    )
    sums = call(
        crossing_sums,
        [((EIGS, 2 * EIGS), F32)],
        (sums, *own, *lend, *ahead, *behind),
        scalars=False,
    )[0]
    reach = 1
    while reach < devices:
        sums = sums + lax.ppermute(sums, AXES, [(i, i ^ reach) for i in range(devices)])
        reach *= 2
    basis, rayleigh = call(
        finish, [((EIGS, width), F32), ((EIGS, EIGS), F32)], (sums, stack), scalars=False
    )
    return basis, rayleigh


def solution(mesh):
    finer = Mesh(mesh.devices.reshape(4, 2, 4, 4), AXES)
    in_specs = (
        P(None, AXES),
        P(AXES, None, None),
        P(AXES),
        P(AXES),
        P(AXES),
        P(AXES, None, None),
        P(AXES),
        P(AXES),
        P(AXES),
    )
    return jax.shard_map(
        shards, mesh=finer, in_specs=in_specs, out_specs=(P(None, AXES), P()), check_vma=False
    )
```

```python
import jax
import jax.numpy as jnp
from jax import lax
from jax.experimental import pallas as pl
from jax.experimental.pallas import tpu as pltpu
from jax.sharding import Mesh
from jax.sharding import PartitionSpec as P

EIGS = 64
TILE = 128
BR_DEV = 64
SLOTS = 64
HALF = 32
CHUNK = 32
PANEL = 1024
AXES = ("grp_0", "grp_1", "row_0", "row_1")
F32 = jnp.float32
BF16 = jnp.bfloat16
VM = pl.BlockSpec(memory_space=pltpu.VMEM)
SM = pl.BlockSpec(memory_space=pltpu.SMEM)
ANY = pl.BlockSpec(memory_space=pl.ANY)
PARAMS = pltpu.CompilerParams(vmem_limit_bytes=16 * 1024 * 1024)
NEAR_ROW, NEAR_COL, CROSS_ROW, CROSS_COL, COUNTS = 0, 1, 2, 3, 4
ODD = 2
MIDDLE = BR_DEV * TILE // 2


def call(body, shapes, inputs, scratch=(), aliases=None, scalars=True, after=()):
    specs = [SM if scalars else VM] + [VM] * (len(inputs) - 1)
    specs += [ANY] * (len(after))
    inputs = tuple(inputs) + tuple(after)
    return pl.pallas_call(
        without(body, len(inputs) - len(after), len(after)),
        out_shape=[jax.ShapeDtypeStruct(s, d) for s, d in shapes],
        in_specs=specs,
        out_specs=[VM] * len(shapes),
        scratch_shapes=[pltpu.VMEM(s, d) for s, d in scratch],
        input_output_aliases=aliases or {},
        compiler_params=PARAMS,
        name=body.__name__,
    )(*inputs)


def without(body, at, count):
    def run(*refs):
        body(*refs[:at], *refs[at + count :])

    return run if count else body


def block(i):
    return pl.ds(pl.multiple_of(i * TILE, TILE), TILE)


def dot(a, b):
    return jnp.dot(a, b, preferred_element_type=F32)


def dot_t(a, b):
    return lax.dot_general(a, b, (((1,), (1,)), ((), ())), preferred_element_type=F32)


def over_slots(count, body):
    def chunk(i, carry):
        for u in range(0, CHUNK, 2):
            body(i * CHUNK + u, i * CHUNK + u + 1)
        return carry

    lax.fori_loop(0, (count + CHUNK - 1) // CHUNK, chunk, 0)


def over_panels(body):
    def panel(i, carry):
        body(pl.ds(pl.multiple_of(i * PANEL, PANEL), PANEL))
        return carry

    lax.fori_loop(0, BR_DEV * TILE // PANEL, panel, 0)


def add_pair(acc, to_1, to_2, left_1, left_2, tile_1, tile_2):
    rows = left_1.shape[0]
    both = dot(
        jnp.concatenate([left_1, left_2], axis=0), jnp.concatenate([tile_1, tile_2], axis=1)
    )
    acc[:, block(to_1)] += both[:rows, :TILE]
    acc[:, block(to_2)] += both[rows:, TILE:]


def add_products(idx, count, source, source_at, target, target_at, tiles):
    def pair(t, u):
        add_pair(
            target,
            idx[target_at, t],
            idx[target_at, u],
            source[:, block(idx[source_at, t])],
            source[:, block(idx[source_at, u])],
            tiles[t],
            tiles[u],
        )

    over_slots(count, pair)


def first_lent(idx, cross, source, even_a, odd_a, even_b, odd_b, acc):
    count = idx[COUNTS, 1]
    is_odd = idx[COUNTS, ODD] == 1
    acc[...] = jnp.zeros_like(acc)

    def left(t):
        rows = source[:, block(idx[CROSS_ROW, t])]
        return jnp.where(t < count, rows, jnp.zeros_like(rows))

    def pair(t, u):
        add_pair(
            acc, idx[CROSS_COL, t], idx[CROSS_COL, u], left(t), left(u), cross[t], cross[u]
        )

    over_slots(count, pair)

    def close(s):
        onward = acc[:, s].astype(BF16)
        back = source[:, s]
        even = jnp.where(is_odd, back, onward)
        odd = jnp.where(is_odd, onward, back)
        even_a[:, s], even_b[:, s] = even[:HALF], even[HALF:]
        odd_a[:, s], odd_b[:, s] = odd[:HALF], odd[HALF:]

    over_panels(close)


def prepare(idx, near, cross, near_m, near_t, cross_m, cross_t):
    def some(i, carry):
        for u in range(4):
            t = 4 * i + u
            for which, src, plain, flipped in (
                (0, near, near_m, near_t),
                (1, cross, cross_m, cross_t),
            ):
                tile = src[t]
                tile = jnp.where(t < idx[COUNTS, which], tile, jnp.zeros_like(tile))
                plain[t] = tile
                flipped[t] = tile.T
        return carry

    lax.fori_loop(0, SLOTS // 4, some, 0)


def near_part(idx, near_m, near_t, own, to_row, to_col):
    to_row[...] = jnp.zeros_like(to_row)
    to_col[...] = jnp.zeros_like(to_col)

    def pair(t, u):
        for acc, source_at, target_at, tiles in (
            (to_row, NEAR_COL, NEAR_ROW, near_t),
            (to_col, NEAR_ROW, NEAR_COL, near_m),
        ):
            add_pair(
                acc,
                idx[target_at, t],
                idx[target_at, u],
                own[:, block(idx[source_at, t])],
                own[:, block(idx[source_at, u])],
                tiles[t],
                tiles[u],
            )

    over_slots(idx[COUNTS, 0], pair)

    def close(s):
        to_row[:, s] += to_col[:, s]

    over_panels(close)


def step_body(
    idx, cross_m, cross_t, from_even, from_odd, current, before, new, new_b, ahead, acc, close
):
    count = idx[COUNTS, 1]
    is_odd = idx[COUNTS, ODD] == 1

    def choose(s):
        ahead[:, s] = jnp.where(is_odd, from_odd[:, s], from_even[:, s])

    over_panels(choose)
    add_products(idx, count, ahead, CROSS_COL, new, CROSS_ROW, cross_t)

    def update(s):
        behind = jnp.where(is_odd, from_even[:, s], from_odd[:, s])
        image = new[:, s] + behind.astype(F32)
        following = -0.25 * current[:, s].astype(F32) - image
        if before is None:
            following = following * (1.0 / 0.75)
        else:
            following = following * (2.0 / 0.75) - before[:, s].astype(F32)
        new[:, s] = following
        new_b[:, s] = following.astype(BF16)
        acc[:, s] = jnp.zeros_like(following)

    over_panels(update)
    add_products(idx, count, new_b, CROSS_ROW, acc, CROSS_COL, cross_m)
    close(is_odd)


def close_full(new_b, acc, to_even, to_odd):
    def close(is_odd):
        def panel(s):
            onward = acc[:, s].astype(BF16)
            back = new_b[:, s]
            to_even[:, s] = jnp.where(is_odd, back, onward)
            to_odd[:, s] = jnp.where(is_odd, onward, back)

        over_panels(panel)

    return close


def first_step(
    idx, near_image, cross_m, cross_t, from_even, from_odd, current,
    new, new_b, to_even, to_odd, ahead, acc,
):
    step_body(
        idx, cross_m, cross_t, from_even, from_odd, current, None, new, new_b, ahead, acc,
        close_full(new_b, acc, to_even, to_odd),
    )


def next_step(
    idx, near_image, cross_m, cross_t, from_even, from_odd, current, before,
    new, new_b, to_even, to_odd, ahead, acc,
):
    step_body(
        idx, cross_m, cross_t, from_even, from_odd, current, before, new, new_b, ahead, acc,
        close_full(new_b, acc, to_even, to_odd),
    )


def last_step(
    idx, near_image, cross_m, cross_t, from_even, from_odd, current, before,
    new, new_b, to_even, to_odd, kept, ahead, acc,
):
    def close(is_odd):
        for k in range(0, MIDDLE, PANEL):
            low, high = slice(k, k + PANEL), slice(MIDDLE + k, MIDDLE + k + PANEL)
            onward = acc[:, low].astype(BF16)
            back = new_b[:, high]
            to_even[:, low] = jnp.where(is_odd, back, onward)
            to_odd[:, low] = jnp.where(is_odd, onward, back)
            kept[:, low] = acc[:, high].astype(BF16)

    step_body(
        idx, cross_m, cross_t, from_even, from_odd, current, before, new, new_b, ahead, acc, close
    )


def local_sums(idx, near_m, own_a, own_b, last_a, last_b, out, stack, acc):
    acc[...] = jnp.zeros_like(acc)

    def left(t):
        rows = block(idx[NEAR_ROW, t])
        return jnp.concatenate([own_a[:, rows], own_b[:, rows]], axis=0)

    def pair(t, u):
        add_pair(
            acc, idx[NEAR_COL, t], idx[NEAR_COL, u], left(t), left(u), near_m[t], near_m[u]
        )

    over_slots(idx[COUNTS, 0], pair)
    total = jnp.zeros((3 * EIGS, EIGS), F32)
    for k in range(0, BR_DEV * TILE, PANEL):
        s = slice(k, k + PANEL)
        own = jnp.concatenate([own_a[:, s], own_b[:, s]], axis=0)
        rest = jnp.concatenate([last_a[:, s], last_b[:, s]], axis=0) - own.astype(F32)
        both = jnp.concatenate([own, rest.astype(BF16)], axis=0)
        stack[:, s] = both
        total = total + dot_t(jnp.concatenate([both, acc[:, s].astype(BF16)], axis=0), own)
    half = 0.5 * total[:EIGS]
    out[:, :EIGS] = half + total[EIGS : 2 * EIGS]
    out[:, EIGS:] = half - total[2 * EIGS :]


def crossing_sums(
    idx, sums, own_a, own_b, kept_a, kept_b, even_a, even_b, odd_a, odd_b, out
):
    is_odd = idx[COUNTS, ODD] == 1
    total = jnp.zeros((EIGS, EIGS), F32)
    for k in range(0, MIDDLE, PANEL):
        s = slice(k, k + PANEL)
        even = jnp.concatenate([even_a[:, s], even_b[:, s]], axis=0)
        odd = jnp.concatenate([odd_a[:, s], odd_b[:, s]], axis=0)
        behind = jnp.where(is_odd, even, odd)
        ahead = jnp.where(is_odd, odd, even)
        own = jnp.concatenate([own_a[:, s], own_b[:, s]], axis=0)
        kept = jnp.concatenate([kept_a[:, s], kept_b[:, s]], axis=0)
        total = total + dot_t(behind, own) + dot_t(kept, ahead)
    gram = sums[:, :EIGS]
    inner = sums[:, EIGS:] - total
    out[:, :EIGS] = gram + gram.T
    out[:, EIGS:] = inner + inner.T


def split(x):
    high = x.astype(BF16)
    return high, (x - high.astype(F32)).astype(BF16)


def inverse_factor(gram):
    wide = 2 * EIGS
    rows = lax.broadcasted_iota(jnp.int32, (EIGS, wide), 0)
    lanes = lax.broadcasted_iota(jnp.int32, (EIGS, wide), 1)
    work = jnp.where(lanes < EIGS, gram, (lanes - EIGS == rows).astype(F32))
    work = [work[i : i + 8] for i in range(0, EIGS, 8)]
    below = lax.broadcasted_iota(jnp.int32, (8, wide), 0)
    done = []
    for p in range(EIGS // 8):
        columns = [
            [jnp.broadcast_to(w[:, 8 * p + k : 8 * p + k + 1], (8, wide)) for w in work]
            for k in range(8)
        ]
        for k in range(8):
            pivot = jnp.broadcast_to(columns[k][0][k : k + 1], (8, wide))
            row = jnp.broadcast_to(work[0][k : k + 1], (8, wide))
            scale = 1.0 / pivot
            factors = [c * scale for c in columns[k]]
            factors[0] = jnp.where(below > k, factors[0], 0.0)
            for later in range(k + 1, 8):
                top = jnp.broadcast_to(columns[later][0][k : k + 1], (8, wide))
                columns[later] = [c - f * top for c, f in zip(columns[later], factors)]
            work = [w - f * row for w, f in zip(work, factors)]
        done.append(work[0])
        work = work[1:]
    work = jnp.concatenate(done, axis=0)
    pivots = jnp.sum(jnp.where(lanes == rows, work, 0.0), axis=1, keepdims=True)
    return (work / jnp.sqrt(pivots))[:, EIGS:]


def finish(sums, stack, basis, rayleigh):
    count = 1.0 / float(128 * BR_DEV * TILE)
    inverse = inverse_factor(sums[...] * count)
    high, low = split(inverse)
    left = jnp.concatenate([high, high, low], axis=1)
    for k in range(0, BR_DEV * TILE, PANEL):
        s = slice(k, k + PANEL)
        both = stack[:, s]
        basis[:, s] = dot(left, jnp.concatenate([both, both[:EIGS]], axis=0))
    inner = sums[:, EIGS:] * count
    halfway = jnp.dot(
        inverse, inner, precision=lax.Precision.HIGHEST, preferred_element_type=F32
    )
    rayleigh[...] = lax.dot_general(
        inverse,
        halfway,
        (((1,), (1,)), ((), ())),
        precision=lax.Precision.HIGHEST,
        preferred_element_type=F32,
    )


def shards(
    iterate, near, near_rows, near_cols, near_count, cross, cross_rows, cross_cols, cross_count
):
    devices = lax.axis_size(AXES)
    width = BR_DEV * TILE

    def swap(x, first):
        pairs = [(i, i + 1) for i in range(first, devices - 1, 2)]
        return lax.ppermute(x, AXES, pairs + [(b, a) for a, b in pairs])

    odd = lax.axis_index("row_1") % 2
    counts = jnp.concatenate(
        [near_count, cross_count, odd[None].astype(jnp.int32), jnp.zeros((SLOTS - 3,), jnp.int32)]
    )
    idx = jnp.stack([near_rows, near_cols, cross_rows, cross_cols, counts])

    half = ((HALF, width), BF16)
    quarter = ((HALF, MIDDLE), BF16)
    full = ((HALF, width), F32)
    tiles = ((SLOTS, TILE, TILE), BF16)

    own = [iterate[:HALF], iterate[HALF:]]
    sent = call(first_lent, [half] * 4, (idx, cross, iterate), [((EIGS, width), F32)])
    from_even, from_odd = [None, None], [None, None]
    for h in range(2):
        from_even[h], from_odd[h] = swap(sent[2 * h], 0), swap(sent[2 * h + 1], 1)
    near_m, near_t, cross_m, cross_t = call(prepare, [tiles] * 4, (idx, near, cross))

    def near_image(h):
        return call(near_part, [full], (idx, near_m, near_t, own[h]), [full])[0]

    images = [near_image(0), near_image(1)]
    before, current = [None, None], list(own)
    kept = [None, None]
    scratch = [half, full]
    for step in range(4):
        for h in range(2):
            args = (idx, images[h], cross_m, cross_t, from_even[h], from_odd[h], current[h])
            outs = [full, half, half, half]
            after = (images[1 - h],) if step or h else ()
            if step == 0:
                new, own[h], even, odd = call(first_step, outs, args, scratch, {1: 0}, after=after)
            elif step < 3:
                args = args + (before[h],)
                new, own[h], even, odd = call(next_step, outs, args, scratch, {1: 0}, after=after)
            else:
                args = args + (before[h],)
                outs = [full, half, quarter, quarter, quarter]
                after = after if h == 0 else ()
                new, own[h], even, odd, kept[h] = call(
                    last_step, outs, args, scratch, {1: 0}, after=after
                )
            before[h], current[h] = current[h], new
            from_even[h], from_odd[h] = swap(even, 0), swap(odd, 1)
            if step < 3:
                images[h] = near_image(h)

    sums, stack = call(
        local_sums,
        [((EIGS, 2 * EIGS), F32), ((2 * EIGS, width), BF16)],
        (idx, near_m, *own, *current),
        [((EIGS, width), F32)],
    )
    sums = call(
        crossing_sums,
        [((EIGS, 2 * EIGS), F32)],
        (idx, sums, *own, *kept, *from_even, *from_odd),
    )[0]
    reach = 1
    while reach < devices:
        sums = sums + lax.ppermute(sums, AXES, [(i, i ^ reach) for i in range(devices)])
        reach *= 2
    basis, rayleigh = call(
        finish, [((EIGS, width), F32), ((EIGS, EIGS), F32)], (sums, stack), scalars=False
    )
    return basis, rayleigh


def solution(mesh):
    finer = Mesh(mesh.devices.reshape(4, 2, 4, 4), AXES)
    in_specs = (
        P(None, AXES),
        P(AXES, None, None),
        P(AXES),
        P(AXES),
        P(AXES),
        P(AXES, None, None),
        P(AXES),
        P(AXES),
        P(AXES),
    )
    return jax.shard_map(
        shards, mesh=finer, in_specs=in_specs, out_specs=(P(None, AXES), P()), check_vma=False
    )
```

```python
import jax
import jax.numpy as jnp
from jax import lax
from jax.experimental import pallas as pl
from jax.experimental.pallas import tpu as pltpu
from jax.sharding import Mesh
from jax.sharding import PartitionSpec as P


EIGS = 64
TILE = 128
BR_DEV = 64
SLOTS = 64
HALF = 32
CHUNK = 32
PANEL = 1024
AXES = ("grp_0", "grp_1", "row_0", "row_1")
F32 = jnp.float32
BF16 = jnp.bfloat16
VM = pl.BlockSpec(memory_space=pltpu.VMEM)
SM = pl.BlockSpec(memory_space=pltpu.SMEM)
ANY = pl.BlockSpec(memory_space=pl.ANY)
PARAMS = pltpu.CompilerParams(vmem_limit_bytes=16 * 1024 * 1024)
PACKED = 48
PART = PACKED // 2


def call(body, shapes, scalars, inputs, scratch=(), aliases=None, after=(), kinds=None):
    first = len(scalars)
    lead = first + len(inputs)

    def run(*refs):
        body(*refs[:lead], *refs[lead + len(after) :])

    return pl.pallas_call(
        run,
        out_shape=[jax.ShapeDtypeStruct(s, d) for s, d in shapes],
        in_specs=[SM] * first + [VM] * len(inputs) + [ANY] * len(after),
        out_specs=kinds or [VM] * len(shapes),
        scratch_shapes=[x if kinds else pltpu.VMEM(*x) for x in scratch],
        input_output_aliases={first + i: o for i, o in (aliases or {}).items()},
        compiler_params=PARAMS,
    )(*scalars, *inputs, *after)


def on_odd_device():
    return lax.axis_index("row_1") % 2 == 1


def block(i):
    return pl.ds(pl.multiple_of(i * TILE, TILE), TILE)


def dot(a, b):
    return jnp.dot(a, b, preferred_element_type=F32)


def dot_t(a, b):
    return lax.dot_general(a, b, (((1,), (1,)), ((), ())), preferred_element_type=F32)


def over_slots(body, unroll=CHUNK):
    def chunk(i, carry):
        for u in range(0, unroll, 2):
            body(i * unroll + u, i * unroll + u + 1)
        return carry

    lax.fori_loop(0, SLOTS // unroll, chunk, 0)


def over_panels(body):
    def panel(i, carry):
        body(pl.ds(pl.multiple_of(i * PANEL, PANEL), PANEL))
        return carry

    lax.fori_loop(0, BR_DEV * TILE // PANEL, panel, 0)


def add_pair(acc, to_1, to_2, left_1, left_2, tile_1, tile_2):
    rows = left_1.shape[0]
    both = dot(
        jnp.concatenate([left_1, left_2], axis=0), jnp.concatenate([tile_1, tile_2], axis=1)
    )
    acc[:, block(to_1)] += both[:rows, :TILE]
    acc[:, block(to_2)] += both[rows:, TILE:]


def add_products(source, source_at, target, target_at, tiles, unroll=CHUNK):
    def pair(t, u):
        add_pair(
            target,
            target_at[t],
            target_at[u],
            source[:, block(source_at[t])],
            source[:, block(source_at[u])],
            tiles[t],
            tiles[u],
        )

    over_slots(pair, unroll)


def close_full(new_b, acc, to_even, to_odd):
    is_odd = on_odd_device()

    def panel(s):
        onward = acc[:, s].astype(BF16)
        back = new_b[:, s]
        to_even[:, s] = jnp.where(is_odd, back, onward)
        to_odd[:, s] = jnp.where(is_odd, onward, back)

    over_panels(panel)


def first_lent(rows, cols, counts, cross, source, to_even, to_odd, acc):
    acc[...] = jnp.zeros_like(acc)
    count = counts[0]

    def left(t):
        picked = source[:, block(rows[t])]
        return jnp.where(t < count, picked, jnp.zeros_like(picked))

    def pair(t, u):
        add_pair(acc, cols[t], cols[u], left(t), left(u), cross[t], cross[u])

    over_slots(pair)
    close_full(source, acc, to_even, to_odd)


def prepare(
    near_count, cross_count, cols, near, cross,
    near_m, near_t, cross_m, cross_t, slots, blocks, over, seen_at,
):
    for c in range(SLOTS):
        seen_at[c] = -1
        blocks[c] = 0

    def some(i, used):
        for u in range(4):
            t = 4 * i + u
            for counts, src, plain, flipped in (
                (near_count, near, near_m, near_t),
                (cross_count, cross, cross_m, cross_t),
            ):
                tile = src[t]
                tile = jnp.where(t < counts[0], tile, jnp.zeros_like(tile))
                plain[t] = tile
                flipped[t] = tile.T
            col = cols[t]
            seen = seen_at[col]
            fresh = jnp.logical_and(t < cross_count[0], seen < 0)
            at = jnp.where(fresh, used, seen)
            seen_at[col] = at
            slots[t] = jnp.clip(at, 0, PACKED - 1)
            blocks[jnp.minimum(used, SLOTS - 1)] = jnp.where(fresh, col, 0)
            used = used + fresh.astype(jnp.int32)
        return used

    used = lax.fori_loop(0, SLOTS // 4, some, jnp.int32(0))
    over[...] = jnp.full(over.shape, jnp.where(used > PACKED, 1.0, 0.0), F32)


def near_part(rows, cols, near_m, near_t, own, to_row, to_col):
    to_row[...] = jnp.zeros_like(to_row)
    to_col[...] = jnp.zeros_like(to_col)

    def pair(t, u):
        for acc, source_at, target_at, tiles in (
            (to_row, cols, rows, near_t),
            (to_col, rows, cols, near_m),
        ):
            add_pair(
                acc,
                target_at[t],
                target_at[u],
                own[:, block(source_at[t])],
                own[:, block(source_at[u])],
                tiles[t],
                tiles[u],
            )

    over_slots(pair)

    def close(s):
        to_row[:, s] += to_col[:, s]

    over_panels(close)


def over_blocks(count, body):
    def some(i, carry):
        for u in range(8):
            body(8 * i + u)
        return carry

    lax.fori_loop(0, count // 8, some, 0)


def recur(new, new_b, current, before, behind):
    def update(s):
        image = new[:, s] if behind is None else new[:, s] + behind(s).astype(F32)
        following = -0.25 * current[:, s].astype(F32) - image
        if before is None:
            following = following * (1.0 / 0.75)
        else:
            following = following * (2.0 / 0.75) - before[:, s].astype(F32)
        new[:, s] = following
        new_b[:, s] = following.astype(BF16)

    over_panels(update)


def pack(rows, slots, theirs, cross_m, new_b, to_even, to_odd, acc):
    is_odd = on_odd_device()
    acc[...] = jnp.zeros_like(acc)
    add_products(new_b, rows, acc, slots, cross_m)

    def one(k):
        onward = acc[:, block(k)].astype(BF16)
        back = new_b[:, block(theirs[k])]
        to_even[:, block(k)] = jnp.where(is_odd, back, onward)
        to_odd[:, block(k)] = jnp.where(is_odd, onward, back)

    over_blocks(PACKED, one)


def unpack(rows, slots, theirs, cross_t, from_even, from_odd, new, ahead):
    is_odd = on_odd_device()
    for k in range(0, PACKED * TILE, PANEL):
        s = slice(k, k + PANEL)
        ahead[:, s] = jnp.where(is_odd, from_odd[:, s], from_even[:, s])
    add_products(ahead, slots, new, rows, cross_t)

    def one(k):
        behind = jnp.where(is_odd, from_even[:, block(k)], from_odd[:, block(k)])
        new[:, block(theirs[k])] += behind.astype(F32)

    over_blocks(PACKED, one)


def first_step(
    rows, cols, slots, theirs, near_rows, near_cols,
    near_image, cross_m, cross_t, from_even, from_odd, current, near_m, near_t,
    new, new_b, to_even, to_odd, image, ahead, acc, to_col,
):
    is_odd = on_odd_device()

    def choose(s):
        ahead[:, s] = jnp.where(is_odd, from_odd[:, s], from_even[:, s])

    over_panels(choose)
    add_products(ahead, cols, new, rows, cross_t)

    def behind(s):
        return jnp.where(is_odd, from_even[:, s], from_odd[:, s])

    recur(new, new_b, current, None, behind)
    pack(rows, slots, theirs, cross_m, new_b, to_even, to_odd, acc)
    near_part(near_rows, near_cols, near_m, near_t, new_b, image, to_col)


def next_step(
    rows, slots, theirs, near_rows, near_cols,
    near_image, cross_m, cross_t, from_even, from_odd, current, before, near_m, near_t,
    new, new_b, to_even, to_odd, image, ahead, acc, to_col,
):
    unpack(rows, slots, theirs, cross_t, from_even, from_odd, new, ahead)
    recur(new, new_b, current, before, None)
    pack(rows, slots, theirs, cross_m, new_b, to_even, to_odd, acc)
    near_part(near_rows, near_cols, near_m, near_t, new_b, image, to_col)


def last_step(
    rows, slots, theirs, near_image, cross_m, cross_t, from_even, from_odd, current, before,
    new, new_b, to_even, to_odd, kept_w, kept_y, ahead, acc,
):
    is_odd = on_odd_device()
    unpack(rows, slots, theirs, cross_t, from_even, from_odd, new, ahead)
    recur(new, new_b, current, before, None)
    acc[...] = jnp.zeros_like(acc)
    add_products(new_b, rows, acc, slots, cross_m)

    def one(k):
        onward = acc[:, block(k)].astype(BF16)
        back = new_b[:, block(theirs[k + PART])]
        to_even[:, block(k)] = jnp.where(is_odd, back, onward)
        to_odd[:, block(k)] = jnp.where(is_odd, onward, back)
        kept_w[:, block(k)] = acc[:, block(k + PART)].astype(BF16)
        kept_y[:, block(k)] = new_b[:, block(theirs[k])]

    over_blocks(PART, one)


def plain_step(
    rows, cols, scale, near_image, cross_t, ahead, behind, current, before, new, new_b
):
    add_products(ahead, cols, new, rows, cross_t, 2)

    def update(s):
        image = new[:, s] + behind[:, s].astype(F32)
        following = (-0.25 * current[:, s] - image) * scale[0] - before[:, s]
        new[:, s] = following
        new_b[:, s] = following.astype(BF16)

    over_panels(update)


def plain_near(rows, cols, near_m, near_t, own, out):
    out[...] = jnp.zeros_like(out)
    add_products(own, cols, out, rows, near_t, 2)
    add_products(own, rows, out, cols, near_m, 2)


def plain_lent(rows, cols, cross_m, source, out, acc):
    acc[...] = jnp.zeros_like(acc)
    add_products(source, rows, acc, cols, cross_m, 2)

    def close(s):
        out[:, s] = acc[:, s].astype(BF16)

    over_panels(close)


def local_sums(rows, cols, near_m, own_a, own_b, last_a, last_b, out, stack, acc):
    acc[...] = jnp.zeros_like(acc)

    def left(t):
        at = block(rows[t])
        return jnp.concatenate([own_a[:, at], own_b[:, at]], axis=0)

    def pair(t, u):
        add_pair(acc, cols[t], cols[u], left(t), left(u), near_m[t], near_m[u])

    over_slots(pair)
    total = jnp.zeros((3 * EIGS, EIGS), F32)
    for k in range(0, BR_DEV * TILE, PANEL):
        s = slice(k, k + PANEL)
        own = jnp.concatenate([own_a[:, s], own_b[:, s]], axis=0)
        rest = jnp.concatenate([last_a[:, s], last_b[:, s]], axis=0) - own.astype(F32)
        both = jnp.concatenate([own, rest.astype(BF16)], axis=0)
        stack[:, s] = both
        total = total + dot_t(jnp.concatenate([both, acc[:, s].astype(BF16)], axis=0), own)
    half = 0.5 * total[:EIGS]
    out[:, :EIGS] = half + total[EIGS : 2 * EIGS]
    out[:, EIGS:] = half - total[2 * EIGS :]


def crossing_sums(
    sums, over, kept_wa, kept_wb, kept_ya, kept_yb, even_a, even_b, odd_a, odd_b, out
):
    is_odd = on_odd_device()
    total = jnp.zeros((EIGS, EIGS), F32)
    for k in range(0, PART * TILE, PANEL):
        s = slice(k, k + PANEL)
        even = jnp.concatenate([even_a[:, s], even_b[:, s]], axis=0)
        odd = jnp.concatenate([odd_a[:, s], odd_b[:, s]], axis=0)
        behind = jnp.where(is_odd, even, odd)
        ahead = jnp.where(is_odd, odd, even)
        own = jnp.concatenate([kept_ya[:, s], kept_yb[:, s]], axis=0)
        kept = jnp.concatenate([kept_wa[:, s], kept_wb[:, s]], axis=0)
        total = total + dot_t(behind, own) + dot_t(kept, ahead)
    gram = sums[:, :EIGS]
    inner = sums[:, EIGS:] - total
    out[:EIGS, :EIGS] = gram + gram.T
    out[:EIGS, EIGS:] = inner + inner.T
    out[EIGS:, :] = over[...]


def split(x):
    high = x.astype(BF16)
    return high, (x - high.astype(F32)).astype(BF16)


def inverse_factor(gram):
    wide = 2 * EIGS
    rows = lax.broadcasted_iota(jnp.int32, (EIGS, wide), 0)
    lanes = lax.broadcasted_iota(jnp.int32, (EIGS, wide), 1)
    work = jnp.where(lanes < EIGS, gram, (lanes - EIGS == rows).astype(F32))
    work = [work[i : i + 8] for i in range(0, EIGS, 8)]
    below = lax.broadcasted_iota(jnp.int32, (8, wide), 0)
    done = []
    for p in range(EIGS // 8):
        columns = [
            [jnp.broadcast_to(w[:, 8 * p + k : 8 * p + k + 1], (8, wide)) for w in work]
            for k in range(8)
        ]
        for k in range(8):
            pivot = jnp.broadcast_to(columns[k][0][k : k + 1], (8, wide))
            row = jnp.broadcast_to(work[0][k : k + 1], (8, wide))
            scale = 1.0 / pivot
            factors = [c * scale for c in columns[k]]
            factors[0] = jnp.where(below > k, factors[0], 0.0)
            for later in range(k + 1, 8):
                top = jnp.broadcast_to(columns[later][0][k : k + 1], (8, wide))
                columns[later] = [c - f * top for c, f in zip(columns[later], factors)]
            work = [w - f * row for w, f in zip(work, factors)]
        done.append(work[0])
        work = work[1:]
    work = jnp.concatenate(done, axis=0)
    pivots = jnp.sum(jnp.where(lanes == rows, work, 0.0), axis=1, keepdims=True)
    return (work / jnp.sqrt(pivots))[:, EIGS:]


def finish(sums, stack, basis, rayleigh, again, panels, square, done):
    again[0] = (sums[EIGS, 0] > 0.0).astype(jnp.int32)
    count = 1.0 / float(128 * BR_DEV * TILE)
    inverse = inverse_factor(sums[:EIGS, :] * count)
    high, low = split(inverse)
    left = jnp.concatenate([high, high, low], axis=1)
    copies = []
    for i, k in enumerate(range(0, BR_DEV * TILE, PANEL)):
        s = slice(k, k + PANEL)
        both = stack[:, s]
        panels[:, s] = dot(left, jnp.concatenate([both, both[:EIGS]], axis=0))
        copies.append(pltpu.make_async_copy(panels.at[:, s], basis.at[:, s], done.at[i]))
        copies[-1].start()
    inner = sums[:EIGS, EIGS:] * count
    halfway = jnp.dot(
        inverse, inner, precision=lax.Precision.HIGHEST, preferred_element_type=F32
    )
    square[...] = lax.dot_general(
        inverse,
        halfway,
        (((1,), (1,)), ((), ())),
        precision=lax.Precision.HIGHEST,
        preferred_element_type=F32,
    )
    copies.append(pltpu.make_async_copy(square, rayleigh, done.at[len(copies)]))
    copies[-1].start()
    for copy in copies:
        copy.wait()


def shards(
    iterate, near, near_rows, near_cols, near_count, cross, cross_rows, cross_cols, cross_count
):
    devices = lax.axis_size(AXES)
    width = BR_DEV * TILE

    def swap(x, first):
        pairs = [(i, i + 1) for i in range(first, devices - 1, 2)]
        return lax.ppermute(x, AXES, pairs + [(b, a) for a, b in pairs])

    near_at = (near_rows, near_cols)
    cross_at = (cross_rows, cross_cols)

    half = ((HALF, width), BF16)
    packed = ((HALF, PACKED * TILE), BF16)
    part = ((HALF, PART * TILE), BF16)
    full = ((HALF, width), F32)
    tiles = ((SLOTS, TILE, TILE), BF16)
    places = ((SLOTS,), jnp.int32)
    table = ((EIGS, 2 * EIGS), F32)

    own = [iterate[:HALF], iterate[HALF:]]
    from_even, from_odd = [None, None], [None, None]

    def ready(counts, cross_to):
        return call(
            prepare,
            [tiles] * 4 + [places, places, ((8, 2 * EIGS), F32)],
            (*counts, cross_to[1]),
            (near, cross),
            [pltpu.SMEM((SLOTS,), jnp.int32)],
            kinds=[VM] * 4 + [SM, SM, VM],
        )

    def exchange(h, even, odd):
        from_odd[h] = swap(odd, 1)
        from_even[h] = swap(even, 0)

    def first_exchange(h, after):
        even, odd = call(
            first_lent,
            [half] * 2,
            (*cross_at, cross_count),
            (cross, own[h]),
            [full],
            after=after,
        )
        exchange(h, even, odd)

    def near_image(h):
        return call(near_part, [full], near_at, (near_m, near_t, own[h]), [full])[0]

    first_exchange(0, ())
    near_m, near_t, cross_m, cross_t, slots, blocks, over = ready(
        (near_count, cross_count), cross_at
    )
    theirs = lax.ppermute(blocks, AXES, [(i, i + 1) for i in range(devices - 1)])
    images = [near_image(0), None]
    first_exchange(1, (images[0],))
    images[1] = near_image(1)
    before, current = [None, None], list(own)
    kept_w, kept_y = [None, None], [None, None]
    for step in range(4):
        for h in range(2):
            args = (images[h], cross_m, cross_t, from_even[h], from_odd[h], current[h])
            at = (cross_rows, slots, theirs)
            outs = [full, half, packed, packed, full]
            if step == 0:
                new, own[h], even, odd, images[h] = call(
                    first_step, outs, (*cross_at, slots, theirs, *near_at), (*args, near_m, near_t),
                    [half, (packed[0], F32), full], {0: 0},
                )
            elif step < 3:
                new, own[h], even, odd, images[h] = call(
                    next_step, outs, (*at, *near_at), (*args, before[h], near_m, near_t),
                    [packed, (packed[0], F32), full], {0: 0},
                )
            else:
                new, own[h], even, odd, kept_w[h], kept_y[h] = call(
                    last_step, [full, half, part, part, part, part], at, (*args, before[h]),
                    [packed, (packed[0], F32)], {0: 0},
                )
            before[h], current[h] = current[h], new
            exchange(h, even, odd)

    def local(near_m, own, current):
        return call(
            local_sums,
            [table, ((2 * EIGS, width), BF16)],
            near_at,
            (near_m, *own, *current),
            [((EIGS, width), F32)],
        )

    def across(x, axis, far):
        return lax.ppermute(x, axis, [(i, i ^ far) for i in range(lax.axis_size(axis))])

    def over_all(sums):
        for axis in ("row_1", "row_0", "grp_0"):
            one, two, three = (across(sums, axis, far) for far in (1, 2, 3))
            sums = (sums + two) + (one + three)
        return sums + across(sums, "grp_1", 1)

    def close(sums, stack):
        return pl.pallas_call(
            finish,
            out_shape=[
                jax.ShapeDtypeStruct((EIGS, width), F32),
                jax.ShapeDtypeStruct((EIGS, EIGS), F32),
                jax.ShapeDtypeStruct((1,), jnp.int32),
            ],
            in_specs=[VM, VM],
            out_specs=[ANY, ANY, SM],
            scratch_shapes=[
                pltpu.VMEM((EIGS, width), F32),
                pltpu.VMEM((EIGS, EIGS), F32),
                pltpu.SemaphoreType.DMA((width // PANEL + 1,)),
            ],
            compiler_params=PARAMS,
            name="finish",
        )(sums, stack)

    sums, stack = local(near_m, own, current)
    sums = call(
        crossing_sums,
        [((EIGS + 8, 2 * EIGS), F32)],
        (),
        (sums, over, *kept_w, *kept_y, *from_even, *from_odd),
    )[0]
    sums = over_all(sums)
    basis, rayleigh, again = close(sums, stack)

    def with_whole_blocks(carry):
        tie = carry[0] - 1
        start = jnp.where(tie == 0, iterate, jnp.zeros_like(iterate))
        near_to, cross_to = [[x + tie for x in at] for at in (near_at, cross_at)]
        counts = (near_count + tie, cross_count + tie)
        near_m, near_t, cross_m, cross_t, _, _, _ = ready(counts, cross_to)
        onward = [(i, i + 1) for i in range(devices - 1)]
        back = [(b, a) for a, b in onward]
        wide = ((EIGS, width), F32)
        wide_b = ((EIGS, width), BF16)

        def lend(at, tiles, x):
            return call(plain_lent, [wide_b], at, (tiles, x), [wide])[0]

        def step(i, state):
            scale = jnp.where(i == 0, 1.0 / 0.75, 2.0 / 0.75).astype(F32)[None]
            own, current, before = state
            image = call(plain_near, [wide], near_to, (near_m, near_t, own))[0]
            behind = lax.ppermute(lend(cross_to, cross_m, own), AXES, onward)
            ahead = lax.ppermute(own, AXES, back)
            new, new_b = call(
                plain_step, [wide, wide_b], (*cross_to, scale),
                (image, cross_t, ahead, behind, current, before), (), {0: 0},
            )
            return new_b, new, current

        state = (start, start.astype(F32), jnp.zeros((EIGS, width), F32))
        own, current, _ = lax.fori_loop(0, 4, step, state)
        stack = jnp.concatenate([own, (current - own.astype(F32)).astype(BF16)], axis=0)
        total = dot_t(jnp.concatenate([stack, lend(near_to, near_m, own)], axis=0), own)
        half_gram = 0.5 * total[:EIGS]
        ahead = lax.ppermute(own, AXES, back)
        inner = half_gram - total[2 * EIGS :] - dot_t(lend(cross_to, cross_m, own), ahead)
        gram = half_gram + total[EIGS : 2 * EIGS]
        sums = jnp.concatenate([gram + gram.T, inner + inner.T], axis=1)
        sums = lax.psum(sums, AXES)
        basis, rayleigh, _ = close(jnp.pad(sums, ((0, 8), (0, 0))), stack)
        return jnp.int32(2), basis, rayleigh

    state = (again[0], basis, rayleigh)
    _, basis, rayleigh = lax.while_loop(lambda c: c[0] == 1, with_whole_blocks, state)
    return basis, rayleigh


def solution(mesh):
    finer = Mesh(mesh.devices.reshape(4, 2, 4, 4), AXES)
    in_specs = (
        P(None, AXES),
        P(AXES, None, None),
        P(AXES),
        P(AXES),
        P(AXES),
        P(AXES, None, None),
        P(AXES),
        P(AXES),
        P(AXES),
    )
    return jax.shard_map(
        shards, mesh=finer, in_specs=in_specs, out_specs=(P(None, AXES), P()), check_vma=False
    )
```
